32 devices in a mesh: row: 4 (over z), col: 8 (over y, x, core).
Axes of the slice: x: 2, y: 2, z: 4, core: 2. Of those that a mesh axis runs over, the one named last changes fastest.
Arguments:
- region: float32 [8, 1024, 8, 1024], P(None, 'col', None, 'row'), may hold values from -6 to 6
- l_panels: bfloat16 [3, 1024, 11, 1024], P(None, 'col', None, 'row'), may hold values from -0.0625 to 0.0625
- u_panels: bfloat16 [3, 11, 1024, 1024], P(None, None, 'col', 'row'), may hold values from -0.0625 to 0.0625
- diag_inv: float32 [3, 1024, 1024], P(None, 'col', 'row'), may hold values from -6 to 6
- pattern: int32 [3, 11, 8], replicated, may hold values from 0 to 1, as said below
Outputs:
- inverse: float32 [11, 1024, 11, 1024], P(None, 'col', None, 'row')
The draws below stay inside these ranges and needn't reach their ends.
Inputs may be any that keep to these rules, and one draw needn't show every extreme that they name: pattern[s] marks the 128-row blocks in the structure of supernode s: only blocks of segments after s; for the last supernode only blocks of the ancestor region; for every other supernode all blocks of one later supernode (its parent in the elimination tree) and otherwise only blocks that the parent's pattern also marks.
All inputs are finite; a program needn't handle non-finite values.
Results may differ from the reference program's by a relative error of at most 0.0003.
Values may be sent and summed in bfloat16 or wider, within the bound.
No kernel may reach another device: no remote copies, remote signals or barrier semaphores. Data moves between devices by JAX's collectives and lax.ppermute only.
A program may use at most 128 MiB of HBM per device.

```python
import jax
import jax.numpy as jnp
from jax import lax

W = 1024
BLK = 128
NSUP = 3
ASEG = 8
NSEG = 11
WB = 8


def draw_pattern(key, part):
    seg_index = jnp.arange(NSEG, dtype=jnp.int32)[:, None] * jnp.ones((1, WB), jnp.int32)
    structs = jnp.zeros((NSUP, NSEG, WB), jnp.int32)
    region_bits = jax.random.randint(jax.random.fold_in(key, 7), (NSEG, WB), 0, 2)
    structs = structs.at[NSUP - 1].set(region_bits * (seg_index >= NSUP).astype(jnp.int32))
    for level in range(NSUP - 2, -1, -1):
        parent = jax.random.randint(jax.random.fold_in(key, 100 + level), (), level + 1, NSUP)
        kept_bits = (jax.random.randint(jax.random.fold_in(key, 200 + level), (NSEG, WB), 0, 4) > 0).astype(jnp.int32)
        parent_blocks = (seg_index == parent).astype(jnp.int32)
        structs = structs.at[level].set(jnp.maximum(parent_blocks, structs[parent] * kept_bits))
    return structs


def steps_of(stream_key, shape, cuts, smallest, top_value):
    def one(position, parts):
        heights = jax.random.uniform(jax.random.fold_in(jax.random.fold_in(stream_key, 6), position), (parts,), jnp.float32, smallest / len(cuts), top_value / len(cuts))
        return jnp.repeat(jnp.exp(heights), shape[position] // parts).reshape((-1,) + (1,) * (len(shape) - position - 1))

    gain = one(*cuts[0])
    for cut in cuts[1:]:
        gain = gain * one(*cut)
    return gain


def bell_draw(stream_key, shape, width, bound, shards=(), kind=jnp.bfloat16):
    loudness = steps_of(stream_key, shape, shards, -0.22, 0.18) if shards else 1.0
    entries = jax.random.normal(stream_key, shape, jnp.float32) * width * loudness
    return jnp.minimum(jnp.maximum(entries, -bound), bound).astype(kind)


def setup_inputs(seed: int = 0) -> dict:
    streams_of = jax.random.split(jax.random.key(seed), 6)
    return {
        "region": bell_draw(streams_of[0], (ASEG, W, ASEG, W), 1.0, 6.0, ((1, 8), (3, 4)), jnp.float32),
        "l_panels": bell_draw(streams_of[1], (NSUP, W, NSEG, W), (ASEG * W) ** -0.5, 0.0625, ((1, 8), (3, 4))),
        "u_panels": bell_draw(streams_of[2], (NSUP, NSEG, W, W), (ASEG * W) ** -0.5, 0.0625, ((2, 8), (3, 4))),
        "diag_inv": bell_draw(streams_of[3], (NSUP, W, W), 1.0, 6.0, ((1, 8), (2, 4)), jnp.float32),
        "pattern": draw_pattern(jax.random.fold_in(streams_of[5], 71), 0),
    }


def reference(region, l_panels, u_panels, diag_inv, pattern):
    inverse = jnp.zeros((NSEG, W, NSEG, W), jnp.float32)
    inverse = inverse.at[NSUP:, :, NSUP:, :].set(region.astype(jnp.float32))
    block_mask = jnp.repeat(pattern.astype(jnp.float32), BLK, axis=2)
    for level in reversed(range(NSUP)):
        mask_now = block_mask[level]
        lower = l_panels[level].astype(jnp.float32) * mask_now[None, :, :]
        upper = u_panels[level].astype(jnp.float32) * mask_now[:, :, None]
        column = -mask_now[:, :, None] * jnp.einsum("ajbk,wbk->ajw", inverse, lower, precision=lax.Precision.HIGHEST)
        row_panel = -mask_now[None, :, :] * jnp.einsum("akw,akbj->wbj", upper, inverse, precision=lax.Precision.HIGHEST)
        diagonal = diag_inv[level] - jnp.einsum("akw,akv->wv", upper, column, precision=lax.Precision.HIGHEST)
        inverse = inverse.at[:, :, level, :].set(column)
        inverse = inverse.at[level].set(row_panel)
        inverse = inverse.at[level, :, level, :].set(diagonal)
    return inverse
```

```python
import functools
import jax
import jax.numpy as jnp
from jax import lax
from jax.experimental import pallas as pl
from jax.experimental.pallas import tpu as pltpu
from jax.sharding import PartitionSpec as P

BLK = 128


F32 = jnp.float32
BF16 = jnp.bfloat16


SMALL, LARGE = 24 * 2**20, 60 * 2**20
TOP = 32760.0
CODES = 16


def pick(x, i, axis=0):
    return lax.dynamic_index_in_dim(x, i, axis, keepdims=False)


def after(x, first):
    return lax.optimization_barrier((x, first))[0]


def put_two(out, at, x):
    hi = x.astype(BF16)
    low = slice(at.start + out.shape[0] // 2, at.stop + out.shape[0] // 2)
    return hi, (x - hi.astype(F32)).astype(BF16), low


def halves_nt(x, b):
    z = dot_nt(x, b)
    n = z.shape[0] // 2
    return z[:n] + z[n:]


def dot_nt(a, b):
    return lax.dot_general(a, b, (((1,), (1,)), ((), ())), preferred_element_type=F32)


def dot_nn(a, b):
    return lax.dot_general(a, b, (((1,), (0,)), ((), ())), preferred_element_type=F32)


def encode(x):
    peak = jnp.maximum(jnp.max(jnp.abs(x), axis=0, keepdims=True), 1e-30)
    code = jnp.ceil(jnp.log2(peak) * 128.0)
    q = jnp.round(x * (TOP * jnp.exp2(code * (-1.0 / 128.0))))
    return q.astype(jnp.int32).astype(jnp.int16), code.astype(jnp.int32)


def scale_of(code16):
    return jnp.exp2(code16.astype(jnp.int32).astype(F32) * (1.0 / 128.0)) * (1.0 / TOP)


def put_coded(out, at, x):
    n = x.shape[0]
    q, code = encode(x)
    out[at + (slice(0, n),)] = q
    out[at + (slice(n, n + CODES),)] = jnp.broadcast_to(code, (CODES, x.shape[1])).astype(jnp.int16)


def decode(ref, at, n, part=None):
    part = part or slice(0, n)
    return ref[at + (part,)].astype(jnp.int32).astype(F32) * scale_of(ref[at + (slice(n, n + 1),)])


def col_share(acc, low, region, pieces, dims):
    base_k, base_l, rows, cols = dims
    acc[:base_k, :] = halves_nt(region[...], low[0, :, :base_l])
    nrow, ncol = base_k, base_l
    for c, q, d in pieces:
        w = low[0, :, ncol : ncol + cols]
        acc[:nrow, :] += halves_nt(c[...], w)
        acc[nrow : nrow + rows, :] = halves_nt(q[...], low[0, :, :ncol]) + halves_nt(d[...], w)
        nrow, ncol = nrow + rows, ncol + cols


def col_body(chunk, *refs, steps, dims, coded):
    pieces = [refs[1 + 3 * i : 4 + 3 * i] for i in range(steps)]
    low, out = refs[1 + 3 * steps : 3 + 3 * steps]
    sends = refs[3 + 3 * steps :]
    acc = out.at[0]
    col_share(acc, low, refs[0], pieces, dims)
    for i in range(coded):

        @pl.when(pl.program_id(0) == i)
        def _():
            put_coded(sends[i], (), acc[...])


def pass_body(share, arrived, out):
    n = share.shape[1]
    put_coded(out, (), share[0] + decode(arrived, (), n))


def col_end_body(keep, share, up, down, x, x_two, *, level, rows):
    n = share.shape[1]
    total = share[0] + decode(up, (), n) + decode(down, (), n)
    for i in range(n // rows):
        here = slice(i * rows, (i + 1) * rows)
        part = jnp.where(keep[level, i] > 0, -total[here, :], 0.0)
        x[here, :] = part
        hi, lo, low = put_two(x_two, here, part)
        x_two[here, :] = hi
        x_two[low, :] = lo


def row_body(here, *refs, steps, dims, n_row, base_tiles):
    base_k, _, rows, cols = dims
    ring = refs[: 2 * n_row - 1]
    piece, downs, ups = ring[0], ring[1:n_row], ring[n_row:]
    r_hi, r_lo = refs[2 * n_row - 1 : 2 * n_row + 1]
    pieces = [refs[2 * n_row + 1 + 3 * i : 2 * n_row + 4 + 3 * i] for i in range(steps)]
    send, mine, up, acc = refs[2 * n_row + 1 + 3 * steps :]

    def twice(at):
        v = up[:, at : at + rows]
        return jnp.concatenate([v, v], axis=1)

    tile_at = pl.program_id(0)

    @pl.when(tile_at == 0)
    def _():
        for j in range(n_row):
            at = here[0] + j
            wraps = at >= n_row
            at = jnp.where(wraps, at - n_row, at)
            dst = pl.ds(pl.multiple_of(at * cols, cols), cols)
            if j == 0:
                up[dst, :] = piece[...]
                continue

            @pl.when(jnp.logical_not(wraps))
            def _():
                up[dst, :] = downs[j - 1][...]

            @pl.when(wraps)
            def _():
                up[dst, :] = ups[n_row - j - 1][...]

    @pl.when(tile_at < base_tiles)
    def _():
        u = up[:, :base_k]
        total = dot_nn(u, r_hi[...]) + dot_nn(u, r_lo[...])
        for i, p in enumerate(pieces):
            total += dot_nn(twice(base_k + i * rows), p[1][...])
        acc[...] = total

    for i in range(steps):

        @pl.when(tile_at == base_tiles + i)
        def _():
            c, _, d = pieces[i]
            nrow = base_k + i * rows
            u = up[:, :nrow]
            total = dot_nn(u, c[:nrow, :]) + dot_nn(u, c[nrow:, :]) + dot_nn(twice(nrow), d[...])
            for j in range(i + 1, steps):
                total += dot_nn(twice(base_k + j * rows), pieces[j][1][...])
            acc[...] = total

    for i in range(send.shape[0]):
        other = pl.ds(pl.multiple_of((2 * i + 1 - here[1]) * rows, rows), rows)
        same = pl.ds(pl.multiple_of((2 * i + here[1]) * rows, rows), rows)
        put_coded(send, (i,), acc[other, :])
        mine[i] = acc[same, :]


def join_body(mine, got, out):
    rows = mine.shape[1]
    put_coded(out, (0,), mine[0] + decode(got, (0,), rows))


def diag_body(up, x_two, out, *, rows):
    n = x_two.shape[0] // 2
    z = dot_nn(up[...], x_two[:n, :]) + dot_nn(up[...], x_two[n:, :])
    for c in range(out.shape[0]):
        put_coded(out, (c,), z[c * rows : (c + 1) * rows, :])


def row_end_body(keep, arrived, y, y_two, *, level, rows, blk):
    for j in range(y.shape[1] // blk):
        at = slice(j * blk, (j + 1) * blk)
        total = jnp.zeros((rows, blk), F32)
        for i in range(arrived.shape[0]):
            code = arrived[i, rows : rows + 1, at]
            total += arrived[i, :rows, at].astype(jnp.int32).astype(F32) * scale_of(code)
        total = jnp.where(keep[level, j] > 0, -total, 0.0)
        y[:, at] = total
        y_two[:rows, at], y_two[rows:, at], _ = put_two(y_two, slice(0, rows), total)


def diag_end_body(start, arrived, d, d_two, *, rows):
    total = start[...]
    for i in range(arrived.shape[0]):
        total -= decode(arrived, (i,), rows)
    d[...] = total
    d_two[:rows, :], d_two[rows:, :], _ = put_two(d_two, slice(0, rows), total)


def pack_region_body(meta, src, out, *, blocks, halves, blk):
    for j in range(blocks):
        seg, at = meta[1, j], 0
        if halves > 1:
            at = pl.multiple_of(meta[2, j] * blk, blk)
        x = src[0, seg, :, pl.ds(at, blk)]
        top = x.astype(BF16)
        out[0, :, j * blk : (j + 1) * blk] = top
        out[1, :, j * blk : (j + 1) * blk] = (x - top.astype(F32)).astype(BF16)


def pack_lower_body(meta, keep, src, out, *, blocks, halves, blk, nsup):
    level = pl.program_id(0)
    for j in range(blocks):
        at = 0
        if halves > 1:
            at = pl.multiple_of(meta[2, j] * blk, blk)
        x = src[0, nsup + meta[1, j], :, pl.ds(at, blk)]
        out[0, :, j * blk : (j + 1) * blk] = jnp.where(keep[level, j] > 0, x, jnp.zeros_like(x))
    base = blocks * blk
    for t in range(1, nsup):
        for h in range(halves):
            x = src[0, t, :, h * blk : (h + 1) * blk]
            at = (nsup - 1 - t) * halves + h
            ok = keep[level, blocks + at] > 0
            at = base + at * blk
            out[0, :, at : at + blk] = jnp.where(ok, x, jnp.zeros_like(x))


def pack_upper_body(meta, keep, src, out, *, level, segs, nsup):
    rows = src.shape[2]
    for i in range(segs + nsup - 1 - level):
        x = src[0, nsup + meta[0, i]] if i < segs else src[0, nsup - 1 - (i - segs)]
        x = jnp.where(keep[level, i] > 0, x.astype(F32), 0.0)
        out[:, i * rows : (i + 1) * rows] = x.T.astype(BF16)


def put_rows_body(meta, *refs, blocks, halves, blk, nsup, nseg, segs, rows):
    xs, ys, ds = refs[:nsup], refs[nsup : 2 * nsup], refs[2 * nsup : 3 * nsup]
    out = refs[-1]
    base_l = blocks * blk
    cols = halves * blk
    for s in range(nsup):

        @pl.when(pl.program_id(0) == s)
        def _():
            for t in range(nsup):
                if t == s:
                    out[0, t] = ds[s][...]
                elif t > s:
                    at = base_l + (nsup - 1 - t) * cols
                    out[0, t] = ys[s][:, at : at + cols]
                else:
                    at = (segs + nsup - 1 - s) * rows
                    out[0, t] = xs[t][at : at + rows, :]
            out[0, nsup:] = jnp.zeros((nseg - nsup,) + out.shape[2:], F32)
            for j in range(blocks):
                at = 0
                if halves > 1:
                    at = pl.multiple_of(meta[2, j] * blk, blk)
                out[0, nsup + meta[1, j], :, pl.ds(at, blk)] = ys[s][:, j * blk : (j + 1) * blk]


def put_cols_body(meta, *refs, segs, nsup, rows):
    out = refs[-1]
    slot = meta[3, pl.program_id(0)]
    here = pl.ds(pl.multiple_of(jnp.minimum(slot, segs - 1) * rows, rows), rows)
    for s in range(nsup):
        x = refs[s][here, :]
        out[0, s] = jnp.where(slot < segs, x, jnp.zeros_like(x))


def chain_gather(piece, n):
    up = down = piece
    ups, downs = [], []
    for step in range(1, n):
        up = lax.ppermute(up, "row", [(i, i + 1) for i in range(step - 1, n - 1)])
        down = lax.ppermute(down, "row", [(i, i - 1) for i in range(1, n - step + 1)])
        ups.append(up)
        downs.append(down)
    return [piece] + downs + ups


def whole(x):
    return pl.BlockSpec(x.shape, lambda *_: (0,) * x.ndim)


def call(body, grid, scalars, inputs, outs, scratch=(), alias=None, limit=SMALL):
    return pl.pallas_call(
        body,
        grid_spec=pltpu.PrefetchScalarGridSpec(
            num_scalar_prefetch=len(scalars),
            grid=grid,
            in_specs=[spec or whole(x) for x, spec in inputs],
            out_specs=[spec or whole(x) for x, spec in outs],
            scratch_shapes=list(scratch),
        ),
        out_shape=[x for x, _ in outs],
        input_output_aliases=alias or {},
        compiler_params=pltpu.CompilerParams(vmem_limit_bytes=limit),
    )(*scalars, *[x for x, _ in inputs])


def branch(region, l_t, u_panels, diag_inv, meta, pattern, cblk, rblk, *, sizes, segs, blocks):
    n_row, n_col, halves, blk = sizes
    nsup, nseg, rows, cols = u_panels.shape
    aseg, last = nseg - nsup, nsup - 1
    n_half = n_col // 2
    row_at, col_at = lax.axis_index("row"), lax.axis_index("col")
    bit = col_at & 1
    base_k, base_l = segs * rows, blocks * blk
    lw = base_l + last * cols
    shape = jax.ShapeDtypeStruct
    sup_ids = jnp.arange(last, 0, -1)
    keep_rows = pick(pattern, cblk, 2)[:, jnp.concatenate([nsup + meta[0, :segs], sup_ids])]
    pat_cols = lax.dynamic_slice_in_dim(pattern, rblk, halves, 2)
    keep_cols = jnp.concatenate(
        [pat_cols[:, nsup + meta[1, :blocks], meta[2, :blocks]], pat_cols[:, sup_ids].reshape(nsup, -1)], 1
    )
    level_spec = pl.BlockSpec((1, nseg, rows, cols), lambda s, *_: (s, 0, 0, 0))

    def upper_piece(s):
        return call(
            functools.partial(pack_upper_body, level=s, segs=segs, nsup=nsup),
            (1,),
            (meta, keep_rows),
            [(u_panels, pl.BlockSpec((1, nseg, rows, cols), lambda i, *_: (s, 0, 0, 0)))],
            [(shape((cols, (segs + last - s) * rows), BF16), None)],
        )[0]

    upper = upper_piece(last)
    ups = {last: chain_gather(upper, n_row)}
    (lower,) = call(
        functools.partial(pack_lower_body, blocks=blocks, halves=halves, blk=blk, nsup=nsup),
        (nsup,),
        (meta, keep_cols),
        [(after(l_t, upper), level_spec)],
        [(shape((nsup, rows, lw), BF16), pl.BlockSpec((1, rows, lw), lambda s, *_: (s, 0, 0)))],
    )
    low_last = lax.all_gather(lower[last:, :, :base_l], "col", axis=1, tiled=True)
    low_rest = lax.all_gather(lower[:last], "col", axis=1, tiled=True)
    region_t = after(region, upper).transpose(0, 2, 1, 3)
    out0 = jnp.pad(region_t, ((nsup, 0), (nsup, 0), (0, 0), (0, 0)))
    pair_spec = pl.BlockSpec((2, rows, base_l), lambda i, m: (0, i, 0))
    known = call(
        functools.partial(pack_region_body, blocks=blocks, halves=halves, blk=blk),
        (segs,),
        (meta,),
        [(region_t, pl.BlockSpec((1, aseg, rows, cols), lambda i, m: (m[0, i], 0, 0, 0)))],
        [(shape((2, base_k, base_l), BF16), pair_spec)],
    )
    known = known[0].reshape(2 * base_k, base_l)
    dims = (base_k, base_l, rows, cols)
    base_tiles, width_all = base_l // cols, rows * n_col
    lane = min(cols, 128)
    pieces = []
    xs, ys, ds = {}, {}, {}
    gate = ups[last][1:]

    def level(s, out0, gate):
        steps = last - s
        nrow, ncol = base_k + steps * rows, base_l + steps * cols
        if s:
            ups[s - 1] = chain_gather(after(upper_piece(s - 1), gate), n_row)
        panel, entry = (low_last, 0) if s == last else (low_rest, s)
        parts = [known] + [p for piece in pieces for p in piece]

        def row_part(parts):
            def tiles(k, depth, wide):
                return pl.BlockSpec((depth, cols), lambda t, h: (k, jnp.minimum(t, wide - 1)))

            inputs = [(parts[0], tiles(k, base_k, base_tiles)) for k in range(2)]
            for i in range(steps):
                c, q, d = parts[1 + 3 * i : 4 + 3 * i]
                inputs += [(c, None), (q, tiles(0, 2 * rows, base_tiles + i)), (d, None)]
            chunk = pl.BlockSpec((n_half, rows + CODES, cols), lambda t, h: (0, 0, t))
            keep = pl.BlockSpec((n_half, rows, cols), lambda t, h: (0, 0, t))
            return call(
                functools.partial(row_body, steps=steps, dims=dims, n_row=n_row, base_tiles=base_tiles),
                (base_tiles + steps,),
                (jnp.stack([row_at, bit]).astype(jnp.int32),),
                [(u, None) for u in ups[s]] + inputs,
                [
                    (shape((n_half, rows + CODES, ncol), jnp.int16), chunk),
                    (shape((n_half, rows, ncol), F32), keep),
                    (shape((width_all, nrow), BF16), None),
                ],
                [pltpu.VMEM((width_all, cols), F32)],
                limit=LARGE,
            )

        def col_part(js, coded):
            chunk = jnp.mod(row_at + jnp.array(js), n_row).astype(jnp.int32)
            outs = [
                (shape((len(js), nrow, cols), F32), pl.BlockSpec((1, nrow, cols), lambda i, c: (i, 0, 0)))
            ]
            outs += [(shape((nrow + CODES, cols), jnp.int16), None)] * coded
            return call(
                functools.partial(col_body, steps=steps, dims=dims, coded=coded),
                (len(js),),
                (chunk,),
                [(p, None) for p in parts]
                + [(panel, pl.BlockSpec((1, cols, ncol), lambda i, c: (entry, c[i], 0)))],
                outs,
                limit=LARGE,
            )

        def share_of(j):
            group, i = shares[j]
            return group, pl.BlockSpec((1, nrow, lane), lambda k, *_: (i, 0, k))

        def flow(j, arrived):
            return call(
                pass_body,
                (cols // lane,),
                (),
                [share_of(j), (arrived, pl.BlockSpec((nrow + CODES, lane), lambda k: (0, k)))],
                [
                    (
                        shape((nrow + CODES, cols), jnp.int16),
                        pl.BlockSpec((nrow + CODES, lane), lambda k: (0, k)),
                    )
                ],
            )[0]

        order = [n_row - 1, 1] + list(range(2, n_row - 1)) + [0]
        group, a, b = col_part(order, 2)
        shares = {j: (group, i) for i, j in enumerate(order)}
        for step in range(1, n_row):
            if step > 1:
                a = flow(n_row - step, flow_up)
                b = flow(step, flow_down)
            flow_up = lax.ppermute(a, "row", [(i, i + 1) for i in range(step)])
            flow_down = lax.ppermute(b, "row", [(i, i - 1) for i in range(n_row - step, n_row)])
            if step == 1:
                send, mine, up = row_part(after(parts, (a, b)))
                got = lax.ppermute(send, "col", [(i, i ^ 1) for i in range(n_col)])
        chunk = pl.BlockSpec((1, rows + CODES, ncol), lambda i: (i, 0, 0))
        (half,) = call(
            join_body,
            (n_half,),
            (),
            [(mine, pl.BlockSpec((1, rows, ncol), lambda i: (i, 0, 0))), (got, chunk)],
            [(shape((n_half, rows + CODES, ncol), jnp.int16), chunk)],
        )
        groups = [[i for i in range(n_col) if i % 2 == b] for b in range(2)]
        swapped = lax.all_to_all(half, "col", 0, 0, axis_index_groups=groups)
        if s == last:
            swapped, out0 = lax.optimization_barrier((swapped, out0))
        y, y_two = call(
            functools.partial(row_end_body, level=s, rows=rows, blk=blk),
            (1,),
            (keep_cols,),
            [(swapped, None)],
            [(shape((rows, ncol), F32), None), (shape((2 * rows, ncol), BF16), None)],
        )
        x_spec = pl.BlockSpec((nrow, lane), lambda k, *_: (0, k))
        coded_spec = pl.BlockSpec((nrow + CODES, lane), lambda k, *_: (0, k))
        x, x_two = call(
            functools.partial(col_end_body, level=s, rows=rows),
            (cols // lane,),
            (keep_rows,),
            [share_of(0), (after(flow_up, y), coded_spec), (flow_down, coded_spec)],
            [
                (shape((nrow, cols), F32), x_spec),
                (shape((2 * nrow, cols), BF16), pl.BlockSpec((2 * nrow, lane), lambda k, *_: (0, k))),
            ],
        )
        (share,) = call(
            functools.partial(diag_body, rows=rows),
            (1,),
            (),
            [(up, None), (x_two, None)],
            [(shape((n_col, rows + CODES, cols), jnp.int16), None)],
        )
        share = lax.all_to_all(share, "col", 0, 0)
        d, d_two = call(
            functools.partial(diag_end_body, rows=rows),
            (1,),
            (),
            [(diag_inv[s], None), (share, None)],
            [(shape((rows, cols), F32), None), (shape((2 * rows, cols), BF16), None)],
        )
        xs[s], ys[s], ds[s] = x, y, d
        pieces.append((x_two, y_two, d_two))
        return out0, x

    for s in reversed(range(nsup)):
        out0, gate = level(s, out0, gate)
    xs, ys, ds = ([v[s] for s in range(nsup)] for v in (xs, ys, ds))
    anywhere = pl.BlockSpec(memory_space=pl.ANY)
    full = shape((nseg, nseg, rows, cols), F32)
    (out,) = call(
        functools.partial(
            put_rows_body, blocks=blocks, halves=halves, blk=blk, nsup=nsup, nseg=nseg, segs=segs, rows=rows
        ),
        (nsup,),
        (meta,),
        [(v, None) for v in xs + ys + ds] + [(out0, anywhere)],
        [(full, pl.BlockSpec((1, nseg, rows, cols), lambda s, m: (s, 0, 0, 0)))],
        alias={1 + 3 * nsup: 0},
    )
    (out,) = call(
        functools.partial(put_cols_body, segs=segs, nsup=nsup, rows=rows),
        (aseg,),
        (meta,),
        [(v, None) for v in xs] + [(out, anywhere)],
        [(full, pl.BlockSpec((1, nsup, rows, cols), lambda a, m: (nsup + a, 0, 0, 0)))],
        alias={1 + nsup: 0},
    )
    return out


def per_device(region, l_panels, u_panels, diag_inv, pattern, *, n_row, n_col, fractions):
    aseg, rows, _, cols = region.shape
    nsup, _ = u_panels.shape[:2]
    blk = min(BLK, cols)
    halves = cols // blk
    row_at, col_at = lax.axis_index("row"), lax.axis_index("col")
    cblk = col_at * rows // BLK
    rblk = row_at * cols // BLK
    used = jnp.max(pattern[:, nsup:], axis=0) > 0
    most_rows = jnp.max(jnp.sum(used, axis=0))
    per_row = used.reshape(aseg, n_row, -1)
    most_cols = jnp.max(jnp.sum(per_row, axis=(0, 2)))
    mine_r = pick(used, cblk, 1)
    mine_c = lax.dynamic_slice_in_dim(used, rblk, halves, 1).reshape(-1)
    seg_list = jnp.argsort(jnp.logical_not(mine_r), stable=True).astype(jnp.int32)
    slot_of = jnp.argsort(seg_list).astype(jnp.int32)
    col_list = jnp.argsort(jnp.logical_not(mine_c), stable=True).astype(jnp.int32)
    wide = aseg * halves
    fill = lambda v: jnp.pad(v, (0, wide - v.shape[0]))
    meta = jnp.stack([fill(seg_list), col_list // halves, col_list % halves, fill(slot_of)])
    l_t = l_panels.transpose(0, 2, 1, 3)
    caps = [(-(-aseg * a // 16), -(-wide * b // 16 // halves) * halves) for a, b in fractions]
    fits = [jnp.logical_and(most_rows <= a, most_cols <= b) for a, b in caps]
    choice = len(caps) - 1
    for i in reversed(range(len(caps) - 1)):
        choice = jnp.where(fits[i], i, choice)
    args = (region, l_t, u_panels, diag_inv, meta, pattern, cblk, rblk)
    makes = [
        functools.partial(branch, sizes=(n_row, n_col, halves, blk), segs=a, blocks=b)
        for a, b in caps
    ]
    out = lax.switch(choice, makes, *args) if len(makes) > 1 else makes[0](*args)
    return out.transpose(0, 2, 1, 3)


FRACTIONS = ((12, 12), (14, 12), (16, 16))


def solution(mesh):
    in_specs = (
        P(None, "col", None, "row"),
        P(None, "col", None, "row"),
        P(None, None, "col", "row"),
        P(None, "col", "row"),
        P(),
    )
    body = functools.partial(
        per_device, n_row=mesh.shape["row"], n_col=mesh.shape["col"], fractions=FRACTIONS
    )
    return jax.shard_map(
        body, mesh=mesh, in_specs=in_specs, out_specs=P(None, "col", None, "row"), check_vma=False
    )
```

```python
import functools
import jax
import jax.numpy as jnp
from jax import lax
from jax.experimental import pallas as pl
from jax.experimental.pallas import tpu as pltpu
from jax.sharding import PartitionSpec as P

BLK = 128


F32 = jnp.float32
BF16 = jnp.bfloat16


SMALL, LARGE = 24 * 2**20, 60 * 2**20
TOP = 32760.0
CODES = 16


def pick(x, i, axis=0):
    return lax.dynamic_index_in_dim(x, i, axis, keepdims=False)


def after(x, first):
    return lax.optimization_barrier((x, first))[0]


def put_two(out, at, x):
    hi = x.astype(BF16)
    low = slice(at.start + out.shape[0] // 2, at.stop + out.shape[0] // 2)
    return hi, (x - hi.astype(F32)).astype(BF16), low


def halves_nt(x, b):
    z = dot_nt(x, b)
    n = z.shape[0] // 2
    return z[:n] + z[n:]


def dot_nt(a, b):
    return lax.dot_general(a, b, (((1,), (1,)), ((), ())), preferred_element_type=F32)


def dot_nn(a, b):
    return lax.dot_general(a, b, (((1,), (0,)), ((), ())), preferred_element_type=F32)


def encode(x):
    peak = jnp.maximum(jnp.max(jnp.abs(x), axis=0, keepdims=True), 1e-30)
    code = jnp.ceil(jnp.log2(peak) * 128.0)
    q = jnp.round(x * (TOP * jnp.exp2(code * (-1.0 / 128.0))))
    return q.astype(jnp.int32).astype(jnp.int16), code.astype(jnp.int32)


def scale_of(code16):
    return jnp.exp2(code16.astype(jnp.int32).astype(F32) * (1.0 / 128.0)) * (1.0 / TOP)


def put_coded(out, at, x):
    n = x.shape[0]
    q, code = encode(x)
    out[at + (slice(0, n),)] = q
    out[at + (slice(n, n + CODES),)] = jnp.broadcast_to(code, (CODES, x.shape[1])).astype(jnp.int16)


def decode(ref, at, n, part=None):
    part = part or slice(0, n)
    return ref[at + (part,)].astype(jnp.int32).astype(F32) * scale_of(ref[at + (slice(n, n + 1),)])


def col_body(chunk, *refs, steps, dims, coded):
    _, base_l, _, cols = dims
    region, panels = refs[0], refs[1 : 1 + steps]
    low, out = refs[1 + steps : 3 + steps]
    sends = refs[3 + steps :]
    total = halves_nt(region[...], low[0, :, :base_l])
    for i, c in enumerate(panels):
        total += halves_nt(c[...], low[0, :, base_l + i * cols : base_l + (i + 1) * cols])
    out[0] = total
    for i in range(coded):

        @pl.when(pl.program_id(0) == i)
        def _():
            put_coded(sends[i], (), out[0])


def side_body(*refs, steps, dims):
    _, base_l, rows, cols = dims
    qs, ds, sups = refs[:steps], refs[steps : 2 * steps], refs[2 * steps : 3 * steps - 1]
    low, out = refs[3 * steps - 1 : 3 * steps + 1]
    parts = []
    for i in range(steps):
        ncol = base_l + i * cols
        total = halves_nt(qs[i][...], low[0, :, :ncol]) + halves_nt(ds[i][...], low[0, :, ncol : ncol + cols])
        for k in range(i + 1, steps):
            w = low[0, :, base_l + k * cols : base_l + (k + 1) * cols]
            sup = sups[k - 1]
            hi, lo = sup[i * rows : (i + 1) * rows, :], sup[(k + i) * rows : (k + i + 1) * rows, :]
            total += dot_nt(hi, w) + dot_nt(lo, w)
        parts.append(total)
    put_coded(out, (0,), parts[0] if steps == 1 else jnp.concatenate(parts, 0))


def side_end_body(keep, arrived, x, x_two, *, level, segs, rows):
    n = x.shape[0]
    total = decode(arrived, (0,), n)
    for i in range(1, arrived.shape[0]):
        total += decode(arrived, (i,), n)
    for i in range(n // rows):
        here = slice(i * rows, (i + 1) * rows)
        part = jnp.where(keep[level, segs + i] > 0, -total[here, :], 0.0)
        x[here, :] = part
        hi, lo, low = put_two(x_two, here, part)
        x_two[here, :] = hi
        x_two[low, :] = lo


def pass_body(share, arrived, out):
    n = share.shape[1]
    put_coded(out, (), share[0] + decode(arrived, (), n))


def col_end_body(keep, share, up, down, x, x_two, *, level, rows):
    n = share.shape[1]
    total = share[0] + decode(up, (), n) + decode(down, (), n)
    for i in range(n // rows):
        here = slice(i * rows, (i + 1) * rows)
        part = jnp.where(keep[level, i] > 0, -total[here, :], 0.0)
        x[here, :] = part
        hi, lo, low = put_two(x_two, here, part)
        x_two[here, :] = hi
        x_two[low, :] = lo


def row_body(here, *refs, steps, dims, n_row, base_tiles):
    base_k, _, rows, cols = dims
    ring = refs[: 2 * n_row - 1]
    piece, downs, ups = ring[0], ring[1:n_row], ring[n_row:]
    r_hi, r_lo = refs[2 * n_row - 1 : 2 * n_row + 1]
    at = 2 * n_row + 1
    pieces = [refs[at + 3 * i : at + 3 * i + 3] for i in range(steps)]
    sups = (None,) + refs[at + 3 * steps : at + 4 * steps - 1] if steps else ()
    send, mine, up, acc = refs[-4:]

    def twice(at):
        v = up[:, at : at + rows]
        return jnp.concatenate([v, v], axis=1)

    tile_at = pl.program_id(0)

    @pl.when(tile_at == 0)
    def _():
        for j in range(n_row):
            at = here[0] + j
            wraps = at >= n_row
            at = jnp.where(wraps, at - n_row, at)
            dst = pl.ds(pl.multiple_of(at * cols, cols), cols)
            if j == 0:
                up[dst, :] = piece[...]
                continue

            @pl.when(jnp.logical_not(wraps))
            def _():
                up[dst, :] = downs[j - 1][...]

            @pl.when(wraps)
            def _():
                up[dst, :] = ups[n_row - j - 1][...]

    @pl.when(tile_at < base_tiles)
    def _():
        u = up[:, :base_k]
        total = dot_nn(u, r_hi[...]) + dot_nn(u, r_lo[...])
        for i, p in enumerate(pieces):
            total += dot_nn(twice(base_k + i * rows), p[1][...])
        acc[...] = total

    for i in range(steps):

        @pl.when(tile_at == base_tiles + i)
        def _():
            c, _, d = pieces[i]
            u = up[:, :base_k]
            total = dot_nn(u, c[:base_k, :]) + dot_nn(u, c[base_k:, :])
            total += dot_nn(twice(base_k + i * rows), d[...])
            for k in range(i):
                v = up[:, base_k + k * rows : base_k + (k + 1) * rows]
                total += dot_nn(v, sups[i][k * rows : (k + 1) * rows, :])
                total += dot_nn(v, sups[i][(i + k) * rows : (i + k + 1) * rows, :])
            for j in range(i + 1, steps):
                total += dot_nn(twice(base_k + j * rows), pieces[j][1][...])
            acc[...] = total

    for i in range(send.shape[0]):
        other = pl.ds(pl.multiple_of((2 * i + 1 - here[1]) * rows, rows), rows)
        same = pl.ds(pl.multiple_of((2 * i + here[1]) * rows, rows), rows)
        put_coded(send, (i,), acc[other, :])
        mine[i] = acc[same, :]


def join_body(mine, got, out):
    rows = mine.shape[1]
    put_coded(out, (0,), mine[0] + decode(got, (0,), rows))


def diag_body(up, x_two, *refs, rows):
    out = refs[-1]
    n = x_two.shape[0] // 2
    u = up[:, :n]
    z = dot_nn(u, x_two[:n, :]) + dot_nn(u, x_two[n:, :])
    if len(refs) > 1:
        m = refs[0].shape[0] // 2
        u = up[:, n : n + m]
        z += dot_nn(u, refs[0][:m, :]) + dot_nn(u, refs[0][m:, :])
    for c in range(out.shape[0]):
        put_coded(out, (c,), z[c * rows : (c + 1) * rows, :])


def row_end_body(keep, arrived, y, y_two, *, level, rows, blk):
    for j in range(y.shape[1] // blk):
        at = slice(j * blk, (j + 1) * blk)
        total = jnp.zeros((rows, blk), F32)
        for i in range(arrived.shape[0]):
            code = arrived[i, rows : rows + 1, at]
            total += arrived[i, :rows, at].astype(jnp.int32).astype(F32) * scale_of(code)
        total = jnp.where(keep[level, j] > 0, -total, 0.0)
        y[:, at] = total
        y_two[:rows, at], y_two[rows:, at], _ = put_two(y_two, slice(0, rows), total)


def diag_end_body(start, arrived, d, d_two, *, rows):
    total = start[...]
    for i in range(arrived.shape[0]):
        total -= decode(arrived, (i,), rows)
    d[...] = total
    d_two[:rows, :], d_two[rows:, :], _ = put_two(d_two, slice(0, rows), total)


def pack_region_body(meta, src, out, *, blocks, halves, blk):
    for j in range(blocks):
        seg, at = meta[1, j], 0
        if halves > 1:
            at = pl.multiple_of(meta[2, j] * blk, blk)
        x = src[0, seg, :, pl.ds(at, blk)]
        top = x.astype(BF16)
        out[0, :, j * blk : (j + 1) * blk] = top
        out[1, :, j * blk : (j + 1) * blk] = (x - top.astype(F32)).astype(BF16)


def pack_lower_body(meta, keep, src, out, *, blocks, halves, blk, nsup):
    level = pl.program_id(0)
    for j in range(blocks):
        at = 0
        if halves > 1:
            at = pl.multiple_of(meta[2, j] * blk, blk)
        x = src[0, nsup + meta[1, j], :, pl.ds(at, blk)]
        out[0, :, j * blk : (j + 1) * blk] = jnp.where(keep[level, j] > 0, x, jnp.zeros_like(x))
    base = blocks * blk
    for t in range(1, nsup):
        for h in range(halves):
            x = src[0, t, :, h * blk : (h + 1) * blk]
            at = (nsup - 1 - t) * halves + h
            ok = keep[level, blocks + at] > 0
            at = base + at * blk
            out[0, :, at : at + blk] = jnp.where(ok, x, jnp.zeros_like(x))


def pack_upper_body(meta, keep, src, out, *, level, segs, nsup):
    rows = src.shape[2]
    for i in range(segs + nsup - 1 - level):
        x = src[0, nsup + meta[0, i]] if i < segs else src[0, nsup - 1 - (i - segs)]
        x = jnp.where(keep[level, i] > 0, x.astype(F32), 0.0)
        out[:, i * rows : (i + 1) * rows] = x.T.astype(BF16)


def put_rows_body(meta, *refs, blocks, halves, blk, nsup, nseg, segs, rows):
    ys, ds, sups = refs[:nsup], refs[nsup : 2 * nsup], refs[2 * nsup : 3 * nsup - 1]
    out = refs[-1]
    base_l = blocks * blk
    cols = halves * blk
    for s in range(nsup):

        @pl.when(pl.program_id(0) == s)
        def _():
            for t in range(nsup):
                if t == s:
                    out[0, t] = ds[s][...]
                elif t > s:
                    at = base_l + (nsup - 1 - t) * cols
                    out[0, t] = ys[s][:, at : at + cols]
                else:
                    at = (nsup - 1 - s) * rows
                    out[0, t] = sups[t][at : at + rows, :]
            out[0, nsup:] = jnp.zeros((nseg - nsup,) + out.shape[2:], F32)
            for j in range(blocks):
                at = 0
                if halves > 1:
                    at = pl.multiple_of(meta[2, j] * blk, blk)
                out[0, nsup + meta[1, j], :, pl.ds(at, blk)] = ys[s][:, j * blk : (j + 1) * blk]


def put_cols_body(meta, *refs, segs, nsup, rows):
    out = refs[-1]
    slot = meta[3, pl.program_id(0)]
    here = pl.ds(pl.multiple_of(jnp.minimum(slot, segs - 1) * rows, rows), rows)
    for s in range(nsup):
        x = refs[s][here, :]
        out[0, s] = jnp.where(slot < segs, x, jnp.zeros_like(x))


def chain_gather(piece, n):
    up = down = piece
    ups, downs = [], []
    for step in range(1, n):
        up = lax.ppermute(up, "row", [(i, i + 1) for i in range(step - 1, n - 1)])
        down = lax.ppermute(down, "row", [(i, i - 1) for i in range(1, n - step + 1)])
        ups.append(up)
        downs.append(down)
    return [piece] + downs + ups


def whole(x):
    return pl.BlockSpec(x.shape, lambda *_: (0,) * x.ndim)


def call(body, grid, scalars, inputs, outs, scratch=(), alias=None, limit=SMALL):
    return pl.pallas_call(
        body,
        grid_spec=pltpu.PrefetchScalarGridSpec(
            num_scalar_prefetch=len(scalars),
            grid=grid,
            in_specs=[spec or whole(x) for x, spec in inputs],
            out_specs=[spec or whole(x) for x, spec in outs],
            scratch_shapes=list(scratch),
        ),
        out_shape=[x for x, _ in outs],
        input_output_aliases=alias or {},
        compiler_params=pltpu.CompilerParams(vmem_limit_bytes=limit),
    )(*scalars, *[x for x, _ in inputs])


def branch(region, l_t, u_panels, diag_inv, meta, pattern, cblk, rblk, *, sizes, segs, blocks):
    n_row, n_col, halves, blk = sizes
    nsup, nseg, rows, cols = u_panels.shape
    aseg, last = nseg - nsup, nsup - 1
    n_half = n_col // 2
    row_at, col_at = lax.axis_index("row"), lax.axis_index("col")
    bit = col_at & 1
    base_k, base_l = segs * rows, blocks * blk
    lw = base_l + last * cols
    shape = jax.ShapeDtypeStruct
    sup_ids = jnp.arange(last, 0, -1)
    keep_rows = pick(pattern, cblk, 2)[:, jnp.concatenate([nsup + meta[0, :segs], sup_ids])]
    pat_cols = lax.dynamic_slice_in_dim(pattern, rblk, halves, 2)
    keep_cols = jnp.concatenate(
        [pat_cols[:, nsup + meta[1, :blocks], meta[2, :blocks]], pat_cols[:, sup_ids].reshape(nsup, -1)], 1
    )
    level_spec = pl.BlockSpec((1, nseg, rows, cols), lambda s, *_: (s, 0, 0, 0))

    def upper_piece(s):
        return call(
            functools.partial(pack_upper_body, level=s, segs=segs, nsup=nsup),
            (1,),
            (meta, keep_rows),
            [(u_panels, pl.BlockSpec((1, nseg, rows, cols), lambda i, *_: (s, 0, 0, 0)))],
            [(shape((cols, (segs + last - s) * rows), BF16), None)],
        )[0]

    upper = upper_piece(last)
    ups = {last: chain_gather(upper, n_row)}
    (lower,) = call(
        functools.partial(pack_lower_body, blocks=blocks, halves=halves, blk=blk, nsup=nsup),
        (nsup,),
        (meta, keep_cols),
        [(after(l_t, upper), level_spec)],
        [(shape((nsup, rows, lw), BF16), pl.BlockSpec((1, rows, lw), lambda s, *_: (s, 0, 0)))],
    )
    low_last = lax.all_gather(lower[last:, :, :base_l], "col", axis=1, tiled=True)
    low_rest = lax.all_gather(lower[:last], "col", axis=1, tiled=True)
    region_t = after(region, upper).transpose(0, 2, 1, 3)
    out0 = jnp.pad(region_t, ((nsup, 0), (nsup, 0), (0, 0), (0, 0)))
    pair_spec = pl.BlockSpec((2, rows, base_l), lambda i, m: (0, i, 0))
    known = call(
        functools.partial(pack_region_body, blocks=blocks, halves=halves, blk=blk),
        (segs,),
        (meta,),
        [(region_t, pl.BlockSpec((1, aseg, rows, cols), lambda i, m: (m[0, i], 0, 0, 0)))],
        [(shape((2, base_k, base_l), BF16), pair_spec)],
    )
    known = known[0].reshape(2 * base_k, base_l)
    dims = (base_k, base_l, rows, cols)
    base_tiles, width_all = base_l // cols, rows * n_col
    lane = min(cols, 128)
    pieces = []
    xs, ys, ds, x_sups, sup_twos = {}, {}, {}, {}, {}
    gate = ups[last][1:]

    def level(s, out0, gate):
        steps = last - s
        nrow, ncol = base_k + steps * rows, base_l + steps * cols
        if s:
            ups[s - 1] = chain_gather(after(upper_piece(s - 1), gate), n_row)
        panel, entry = (low_last, 0) if s == last else (low_rest, s)
        cs, qs, dd = ([p[k] for p in pieces] for k in range(3))
        sup_list = [sup_twos[last - i] for i in range(1, steps)]

        def row_part(known, cs, qs, dd, sup_list):
            def tiles(k, depth, wide):
                return pl.BlockSpec((depth, cols), lambda t, h: (k, jnp.minimum(t, wide - 1)))

            inputs = [(known, tiles(k, base_k, base_tiles)) for k in range(2)]
            for i in range(steps):
                inputs += [(cs[i], None), (qs[i], tiles(0, 2 * rows, base_tiles + i)), (dd[i], None)]
            inputs += [(x, None) for x in sup_list]
            chunk = pl.BlockSpec((n_half, rows + CODES, cols), lambda t, h: (0, 0, t))
            keep = pl.BlockSpec((n_half, rows, cols), lambda t, h: (0, 0, t))
            return call(
                functools.partial(row_body, steps=steps, dims=dims, n_row=n_row, base_tiles=base_tiles),
                (base_tiles + steps,),
                (jnp.stack([row_at, bit]).astype(jnp.int32),),
                [(u, None) for u in ups[s]] + inputs,
                [
                    (shape((n_half, rows + CODES, ncol), jnp.int16), chunk),
                    (shape((n_half, rows, ncol), F32), keep),
                    (shape((width_all, nrow), BF16), None),
                ],
                [pltpu.VMEM((width_all, cols), F32)],
                limit=LARGE,
            )

        def col_part(js, coded):
            chunk = jnp.mod(row_at + jnp.array(js), n_row).astype(jnp.int32)
            outs = [
                (shape((len(js), base_k, cols), F32), pl.BlockSpec((1, base_k, cols), lambda i, c: (i, 0, 0)))
            ]
            outs += [(shape((base_k + CODES, cols), jnp.int16), None)] * coded
            return call(
                functools.partial(col_body, steps=steps, dims=dims, coded=coded),
                (len(js),),
                (chunk,),
                [(p, None) for p in [known] + cs]
                + [(panel, pl.BlockSpec((1, cols, ncol), lambda i, c: (entry, c[i], 0)))],
                outs,
                limit=LARGE,
            )

        def share_of(j):
            group, i = shares[j]
            return group, pl.BlockSpec((1, base_k, lane), lambda k, *_: (i, 0, k))

        def flow(j, arrived):
            return call(
                pass_body,
                (cols // lane,),
                (),
                [share_of(j), (arrived, pl.BlockSpec((base_k + CODES, lane), lambda k: (0, k)))],
                [
                    (
                        shape((base_k + CODES, cols), jnp.int16),
                        pl.BlockSpec((base_k + CODES, lane), lambda k: (0, k)),
                    )
                ],
            )[0]

        order = [n_row - 1, 1] + list(range(2, n_row - 1)) + [0]
        group, a, b = col_part(order, 2)
        x_sup = sup_two = None
        if steps:
            (share,) = call(
                functools.partial(side_body, steps=steps, dims=dims),
                (n_row,),
                (),
                [(x, None) for x in qs + after(dd, (a, b)) + sup_list]
                + [(panel, pl.BlockSpec((1, cols, ncol), lambda i: (entry, i, 0)))],
                [
                    (
                        shape((n_row, steps * rows + CODES, cols), jnp.int16),
                        pl.BlockSpec((1, steps * rows + CODES, cols), lambda i: (i, 0, 0)),
                    )
                ],
                limit=LARGE,
            )
            share = lax.all_to_all(share, "row", 0, 0)
            x_sup, sup_two = call(
                functools.partial(side_end_body, level=s, segs=segs, rows=rows),
                (1,),
                (keep_rows,),
                [(share, None)],
                [(shape((steps * rows, cols), F32), None), (shape((2 * steps * rows, cols), BF16), None)],
            )
            x_sups[s], sup_twos[s] = x_sup, sup_two
        shares = {j: (group, i) for i, j in enumerate(order)}
        for step in range(1, n_row):
            if step > 1:
                a = flow(n_row - step, flow_up)
                b = flow(step, flow_down)
            flow_up = lax.ppermute(a, "row", [(i, i + 1) for i in range(step)])
            flow_down = lax.ppermute(b, "row", [(i, i - 1) for i in range(n_row - step, n_row)])
            if step == 1:
                send, mine, up = row_part(after(known, (a, b)), cs, qs, dd, sup_list)
                got = lax.ppermute(send, "col", [(i, i ^ 1) for i in range(n_col)])
        chunk = pl.BlockSpec((1, rows + CODES, ncol), lambda i: (i, 0, 0))
        (half,) = call(
            join_body,
            (n_half,),
            (),
            [(mine, pl.BlockSpec((1, rows, ncol), lambda i: (i, 0, 0))), (got, chunk)],
            [(shape((n_half, rows + CODES, ncol), jnp.int16), chunk)],
        )
        groups = [[i for i in range(n_col) if i % 2 == b] for b in range(2)]
        swapped = lax.all_to_all(half, "col", 0, 0, axis_index_groups=groups)
        y, y_two = call(
            functools.partial(row_end_body, level=s, rows=rows, blk=blk),
            (1,),
            (keep_cols,),
            [(swapped, None)],
            [(shape((rows, ncol), F32), None), (shape((2 * rows, ncol), BF16), None)],
        )
        x_spec = pl.BlockSpec((base_k, lane), lambda k, *_: (0, k))
        coded_spec = pl.BlockSpec((base_k + CODES, lane), lambda k, *_: (0, k))
        x, x_two = call(
            functools.partial(col_end_body, level=s, rows=rows),
            (cols // lane,),
            (keep_rows,),
            [share_of(0), (after(flow_up, y), coded_spec), (flow_down, coded_spec)],
            [
                (shape((base_k, cols), F32), x_spec),
                (shape((2 * base_k, cols), BF16), pl.BlockSpec((2 * base_k, lane), lambda k, *_: (0, k))),
            ],
        )
        (share,) = call(
            functools.partial(diag_body, rows=rows),
            (1,),
            (),
            [(up, None), (x_two, None)] + ([(sup_two, None)] if steps else []),
            [(shape((n_col, rows + CODES, cols), jnp.int16), None)],
        )
        share = lax.all_to_all(share, "col", 0, 0)
        d, d_two = call(
            functools.partial(diag_end_body, rows=rows),
            (1,),
            (),
            [(diag_inv[s], None), (share, None)],
            [(shape((rows, cols), F32), None), (shape((2 * rows, cols), BF16), None)],
        )
        xs[s], ys[s], ds[s] = x, y, d
        pieces.append((x_two, y_two, d_two))
        return out0, x

    for s in reversed(range(nsup)):
        out0, gate = level(s, out0, gate)
    xs, ys, ds = ([v[s] for s in range(nsup)] for v in (xs, ys, ds))
    sups = [x_sups[s] for s in range(last)]
    anywhere = pl.BlockSpec(memory_space=pl.ANY)
    full = shape((nseg, nseg, rows, cols), F32)
    (out,) = call(
        functools.partial(put_cols_body, segs=segs, nsup=nsup, rows=rows),
        (aseg,),
        (meta,),
        [(v, None) for v in xs] + [(out0, anywhere)],
        [(full, pl.BlockSpec((1, nsup, rows, cols), lambda a, m: (nsup + a, 0, 0, 0)))],
        alias={1 + nsup: 0},
    )
    (out,) = call(
        functools.partial(
            put_rows_body, blocks=blocks, halves=halves, blk=blk, nsup=nsup, nseg=nseg, segs=segs, rows=rows
        ),
        (nsup,),
        (meta,),
        [(v, None) for v in ys + ds + sups] + [(out, anywhere)],
        [(full, pl.BlockSpec((1, nseg, rows, cols), lambda s, m: (s, 0, 0, 0)))],
        alias={3 * nsup: 0},
    )
    return out


def per_device(region, l_panels, u_panels, diag_inv, pattern, *, n_row, n_col, fractions):
    aseg, rows, _, cols = region.shape
    nsup, _ = u_panels.shape[:2]
    blk = min(BLK, cols)
    halves = cols // blk
    row_at, col_at = lax.axis_index("row"), lax.axis_index("col")
    cblk = col_at * rows // BLK
    rblk = row_at * cols // BLK
    used = jnp.max(pattern[:, nsup:], axis=0) > 0
    most_rows = jnp.max(jnp.sum(used, axis=0))
    per_row = used.reshape(aseg, n_row, -1)
    most_cols = jnp.max(jnp.sum(per_row, axis=(0, 2)))
    mine_r = pick(used, cblk, 1)
    mine_c = lax.dynamic_slice_in_dim(used, rblk, halves, 1).reshape(-1)
    seg_list = jnp.argsort(jnp.logical_not(mine_r), stable=True).astype(jnp.int32)
    slot_of = jnp.argsort(seg_list).astype(jnp.int32)
    col_list = jnp.argsort(jnp.logical_not(mine_c), stable=True).astype(jnp.int32)
    wide = aseg * halves
    fill = lambda v: jnp.pad(v, (0, wide - v.shape[0]))
    meta = jnp.stack([fill(seg_list), col_list // halves, col_list % halves, fill(slot_of)])
    l_t = l_panels.transpose(0, 2, 1, 3)
    caps = [(-(-aseg * a // 16), -(-wide * b // 16 // halves) * halves) for a, b in fractions]
    fits = [jnp.logical_and(most_rows <= a, most_cols <= b) for a, b in caps]
    choice = len(caps) - 1
    for i in reversed(range(len(caps) - 1)):
        choice = jnp.where(fits[i], i, choice)
    args = (region, l_t, u_panels, diag_inv, meta, pattern, cblk, rblk)
    makes = [
        functools.partial(branch, sizes=(n_row, n_col, halves, blk), segs=a, blocks=b)
        for a, b in caps
    ]
    out = lax.switch(choice, makes, *args) if len(makes) > 1 else makes[0](*args)
    return out.transpose(0, 2, 1, 3)


FRACTIONS = ((12, 12), (14, 12), (16, 16))


def solution(mesh):
    in_specs = (
        P(None, "col", None, "row"),
        P(None, "col", None, "row"),
        P(None, None, "col", "row"),
        P(None, "col", "row"),
        P(),
    )
    body = functools.partial(
        per_device, n_row=mesh.shape["row"], n_col=mesh.shape["col"], fractions=FRACTIONS
    )
    return jax.shard_map(
        body, mesh=mesh, in_specs=in_specs, out_specs=P(None, "col", None, "row"), check_vma=False
    )
```

```python
import functools
import jax
import jax.numpy as jnp
from jax import lax
from jax.experimental import pallas as pl
from jax.experimental.pallas import tpu as pltpu
from jax.sharding import PartitionSpec as P

BLK = 128


F32 = jnp.float32
BF16 = jnp.bfloat16


SMALL, LARGE = 24 * 2**20, 60 * 2**20
TOP = 32760.0
CODES = 16


def pick(x, i, axis=0):
    return lax.dynamic_index_in_dim(x, i, axis, keepdims=False)


def after(x, first):
    return lax.optimization_barrier((x, first))[0]


def put_two(out, at, x):
    hi = x.astype(BF16)
    low = slice(at.start + out.shape[0] // 2, at.stop + out.shape[0] // 2)
    return hi, (x - hi.astype(F32)).astype(BF16), low


def halves_nt(x, b):
    z = dot_nt(x, b)
    n = z.shape[0] // 2
    return z[:n] + z[n:]


def dot_nt(a, b):
    return lax.dot_general(a, b, (((1,), (1,)), ((), ())), preferred_element_type=F32)


def dot_nn(a, b):
    return lax.dot_general(a, b, (((1,), (0,)), ((), ())), preferred_element_type=F32)


def encode(x):
    peak = jnp.maximum(jnp.max(jnp.abs(x), axis=0, keepdims=True), 1e-30)
    code = jnp.ceil(jnp.log2(peak) * 128.0)
    q = jnp.round(x * (TOP * jnp.exp2(code * (-1.0 / 128.0))))
    return q.astype(jnp.int32).astype(jnp.int16), code.astype(jnp.int32)


def scale_of(code16):
    return jnp.exp2(code16.astype(jnp.int32).astype(F32) * (1.0 / 128.0)) * (1.0 / TOP)


def put_coded(out, at, x):
    n = x.shape[0]
    q, code = encode(x)
    out[at + (slice(0, n),)] = q
    out[at + (slice(n, n + CODES),)] = jnp.broadcast_to(code, (CODES, x.shape[1])).astype(jnp.int16)


def decode(ref, at, n, part=None):
    part = part or slice(0, n)
    return ref[at + (part,)].astype(jnp.int32).astype(F32) * scale_of(ref[at + (slice(n, n + 1),)])


def col_body(chunk, *refs, steps, dims, coded):
    _, base_l, _, cols = dims
    region, panels = refs[0], refs[1 : 1 + steps]
    low, out = refs[1 + steps : 3 + steps]
    sends = refs[3 + steps :]
    total = halves_nt(region[...], low[0, :, :base_l])
    for i, c in enumerate(panels):
        total += halves_nt(c[...], low[0, :, base_l + i * cols : base_l + (i + 1) * cols])
    out[0] = total
    for i in range(coded):

        @pl.when(pl.program_id(0) == i)
        def _():
            put_coded(sends[i], (), out[0])


def side_body(*refs, steps, dims):
    _, base_l, rows, cols = dims
    qs, ds, sups = refs[:steps], refs[steps : 2 * steps], refs[2 * steps : 3 * steps - 1]
    low, out = refs[3 * steps - 1 : 3 * steps + 1]
    parts = []
    for i in range(steps):
        ncol = base_l + i * cols
        total = halves_nt(qs[i][...], low[0, :, :ncol]) + halves_nt(ds[i][...], low[0, :, ncol : ncol + cols])
        for k in range(i + 1, steps):
            w = low[0, :, base_l + k * cols : base_l + (k + 1) * cols]
            sup = sups[k - 1]
            hi, lo = sup[i * rows : (i + 1) * rows, :], sup[(k + i) * rows : (k + i + 1) * rows, :]
            total += dot_nt(hi, w) + dot_nt(lo, w)
        parts.append(total)
    put_coded(out, (0,), parts[0] if steps == 1 else jnp.concatenate(parts, 0))


def side_end_body(keep, arrived, x, x_two, *, level, segs, rows):
    n = x.shape[0]
    total = decode(arrived, (0,), n)
    for i in range(1, arrived.shape[0]):
        total += decode(arrived, (i,), n)
    for i in range(n // rows):
        here = slice(i * rows, (i + 1) * rows)
        part = jnp.where(keep[level, segs + i] > 0, -total[here, :], 0.0)
        x[here, :] = part
        hi, lo, low = put_two(x_two, here, part)
        x_two[here, :] = hi
        x_two[low, :] = lo


def pass_body(share, arrived, out):
    n = share.shape[1]
    put_coded(out, (), share[0] + decode(arrived, (), n))


def col_end_body(keep, share, up, down, x, x_two, *, level, rows):
    n = share.shape[1]
    total = share[0] + decode(up, (), n) + decode(down, (), n)
    for i in range(n // rows):
        here = slice(i * rows, (i + 1) * rows)
        part = jnp.where(keep[level, i] > 0, -total[here, :], 0.0)
        x[here, :] = part
        hi, lo, low = put_two(x_two, here, part)
        x_two[here, :] = hi
        x_two[low, :] = lo


def row_body(here, *refs, steps, dims, n_row, base_tiles):
    base_k, _, rows, cols = dims
    ring = refs[: 2 * n_row - 1]
    piece, downs, ups = ring[0], ring[1:n_row], ring[n_row:]
    r_hi, r_lo = refs[2 * n_row - 1 : 2 * n_row + 1]
    at = 2 * n_row + 1
    pieces = [refs[at + 3 * i : at + 3 * i + 3] for i in range(steps)]
    sups = (None,) + refs[at + 3 * steps : at + 4 * steps - 1] if steps else ()
    send, mine, up, acc = refs[-4:]

    def twice(at):
        v = up[:, at : at + rows]
        return jnp.concatenate([v, v], axis=1)

    tile_at = pl.program_id(0)

    @pl.when(tile_at == 0)
    def _():
        for j in range(n_row):
            at = here[0] + j
            wraps = at >= n_row
            at = jnp.where(wraps, at - n_row, at)
            dst = pl.ds(pl.multiple_of(at * cols, cols), cols)
            if j == 0:
                up[dst, :] = piece[...]
                continue

            @pl.when(jnp.logical_not(wraps))
            def _():
                up[dst, :] = downs[j - 1][...]

            @pl.when(wraps)
            def _():
                up[dst, :] = ups[n_row - j - 1][...]

    @pl.when(tile_at < base_tiles)
    def _():
        u = up[:, :base_k]
        total = dot_nn(u, r_hi[...]) + dot_nn(u, r_lo[...])
        for i, p in enumerate(pieces):
            total += dot_nn(twice(base_k + i * rows), p[1][...])
        acc[...] = total

    for i in range(steps):

        @pl.when(tile_at == base_tiles + i)
        def _():
            c, _, d = pieces[i]
            u = up[:, :base_k]
            total = dot_nn(u, c[:base_k, :]) + dot_nn(u, c[base_k:, :])
            total += dot_nn(twice(base_k + i * rows), d[...])
            for k in range(i):
                v = up[:, base_k + k * rows : base_k + (k + 1) * rows]
                total += dot_nn(v, sups[i][k * rows : (k + 1) * rows, :])
                total += dot_nn(v, sups[i][(i + k) * rows : (i + k + 1) * rows, :])
            for j in range(i + 1, steps):
                total += dot_nn(twice(base_k + j * rows), pieces[j][1][...])
            acc[...] = total

    for i in range(send.shape[0]):
        other = pl.ds(pl.multiple_of((2 * i + 1 - here[1]) * rows, rows), rows)
        same = pl.ds(pl.multiple_of((2 * i + here[1]) * rows, rows), rows)
        put_coded(send, (i,), acc[other, :])
        mine[i] = acc[same, :]


def join_body(mine, got, out):
    rows = mine.shape[1]
    put_coded(out, (0,), mine[0] + decode(got, (0,), rows))


def diag_body(up, x_two, *refs, rows):
    out = refs[-1]
    n = x_two.shape[0] // 2
    u = up[:, :n]
    z = dot_nn(u, x_two[:n, :]) + dot_nn(u, x_two[n:, :])
    if len(refs) > 1:
        m = refs[0].shape[0] // 2
        u = up[:, n : n + m]
        z += dot_nn(u, refs[0][:m, :]) + dot_nn(u, refs[0][m:, :])
    for c in range(out.shape[0]):
        put_coded(out, (c,), z[c * rows : (c + 1) * rows, :])


def row_end_body(keep, arrived, y, y_two, *, level, rows, blk):
    for j in range(y.shape[1] // blk):
        at = slice(j * blk, (j + 1) * blk)
        total = jnp.zeros((rows, blk), F32)
        for i in range(arrived.shape[0]):
            code = arrived[i, rows : rows + 1, at]
            total += arrived[i, :rows, at].astype(jnp.int32).astype(F32) * scale_of(code)
        total = jnp.where(keep[level, j] > 0, -total, 0.0)
        y[:, at] = total
        y_two[:rows, at], y_two[rows:, at], _ = put_two(y_two, slice(0, rows), total)


def diag_end_body(start, arrived, d, d_two, *, rows):
    total = start[...]
    for i in range(arrived.shape[0]):
        total -= decode(arrived, (i,), rows)
    d[...] = total
    d_two[:rows, :], d_two[rows:, :], _ = put_two(d_two, slice(0, rows), total)


def pack_region_body(meta, src, out, *, blocks, halves, blk):
    for j in range(blocks):
        seg, at = meta[1, j], 0
        if halves > 1:
            at = pl.multiple_of(meta[2, j] * blk, blk)
        x = src[0, seg, :, pl.ds(at, blk)]
        top = x.astype(BF16)
        out[0, :, j * blk : (j + 1) * blk] = top
        out[1, :, j * blk : (j + 1) * blk] = (x - top.astype(F32)).astype(BF16)


def pack_lower_body(meta, keep, src, out, *, blocks, halves, blk, nsup):
    level = pl.program_id(0)
    for j in range(blocks):
        at = 0
        if halves > 1:
            at = pl.multiple_of(meta[2, j] * blk, blk)
        x = src[0, nsup + meta[1, j], :, pl.ds(at, blk)]
        out[0, :, j * blk : (j + 1) * blk] = jnp.where(keep[level, j] > 0, x, jnp.zeros_like(x))
    base = blocks * blk
    for t in range(1, nsup):
        for h in range(halves):
            x = src[0, t, :, h * blk : (h + 1) * blk]
            at = (nsup - 1 - t) * halves + h
            ok = keep[level, blocks + at] > 0
            at = base + at * blk
            out[0, :, at : at + blk] = jnp.where(ok, x, jnp.zeros_like(x))


def pack_upper_body(meta, keep, src, out, *, level, segs, nsup):
    rows = src.shape[2]
    for i in range(segs + nsup - 1 - level):
        x = src[0, nsup + meta[0, i]] if i < segs else src[0, nsup - 1 - (i - segs)]
        x = jnp.where(keep[level, i] > 0, x.astype(F32), 0.0)
        out[:, i * rows : (i + 1) * rows] = x.T.astype(BF16)


def put_rows_body(meta, *refs, blocks, halves, blk, nsup, nseg, segs, rows):
    ys, ds, sups = refs[:nsup], refs[nsup : 2 * nsup], refs[2 * nsup : 3 * nsup - 1]
    out = refs[-1]
    base_l = blocks * blk
    cols = halves * blk
    for s in range(nsup):

        @pl.when(pl.program_id(0) == s)
        def _():
            for t in range(nsup):
                if t == s:
                    out[0, t] = ds[s][...]
                elif t > s:
                    at = base_l + (nsup - 1 - t) * cols
                    out[0, t] = ys[s][:, at : at + cols]
                else:
                    at = (nsup - 1 - s) * rows
                    out[0, t] = sups[t][at : at + rows, :]
            out[0, nsup:] = jnp.zeros((nseg - nsup,) + out.shape[2:], F32)
            for j in range(blocks):
                at = 0
                if halves > 1:
                    at = pl.multiple_of(meta[2, j] * blk, blk)
                out[0, nsup + meta[1, j], :, pl.ds(at, blk)] = ys[s][:, j * blk : (j + 1) * blk]


def put_cols_body(meta, *refs, segs, nsup, rows):
    out = refs[-1]
    slot = meta[3, pl.program_id(0)]
    here = pl.ds(pl.multiple_of(jnp.minimum(slot, segs - 1) * rows, rows), rows)
    for s in range(nsup):
        x = refs[s][here, :]
        out[0, s] = jnp.where(slot < segs, x, jnp.zeros_like(x))


def chain_gather(piece, n):
    up = down = piece
    ups, downs = [], []
    for step in range(1, n):
        up = lax.ppermute(up, "row", [(i, i + 1) for i in range(step - 1, n - 1)])
        down = lax.ppermute(down, "row", [(i, i - 1) for i in range(1, n - step + 1)])
        ups.append(up)
        downs.append(down)
    return [piece] + downs + ups


def whole(x):
    return pl.BlockSpec(x.shape, lambda *_: (0,) * x.ndim)


def call(body, grid, scalars, inputs, outs, scratch=(), alias=None, limit=SMALL):
    return pl.pallas_call(
        body,
        grid_spec=pltpu.PrefetchScalarGridSpec(
            num_scalar_prefetch=len(scalars),
            grid=grid,
            in_specs=[spec or whole(x) for x, spec in inputs],
            out_specs=[spec or whole(x) for x, spec in outs],
            scratch_shapes=list(scratch),
        ),
        out_shape=[x for x, _ in outs],
        input_output_aliases=alias or {},
        compiler_params=pltpu.CompilerParams(vmem_limit_bytes=limit),
    )(*scalars, *[x for x, _ in inputs])


def branch(region, l_t, u_panels, diag_inv, meta, pattern, cblk, rblk, *, sizes, segs, blocks):
    n_row, n_col, halves, blk = sizes
    nsup, nseg, rows, cols = u_panels.shape
    aseg, last = nseg - nsup, nsup - 1
    n_half = n_col // 2
    row_at, col_at = lax.axis_index("row"), lax.axis_index("col")
    bit = col_at & 1
    base_k, base_l = segs * rows, blocks * blk
    lw = base_l + last * cols
    shape = jax.ShapeDtypeStruct
    sup_ids = jnp.arange(last, 0, -1)
    keep_rows = pick(pattern, cblk, 2)[:, jnp.concatenate([nsup + meta[0, :segs], sup_ids])]
    pat_cols = lax.dynamic_slice_in_dim(pattern, rblk, halves, 2)
    keep_cols = jnp.concatenate(
        [pat_cols[:, nsup + meta[1, :blocks], meta[2, :blocks]], pat_cols[:, sup_ids].reshape(nsup, -1)], 1
    )
    level_spec = pl.BlockSpec((1, nseg, rows, cols), lambda s, *_: (s, 0, 0, 0))

    def upper_piece(s):
        return call(
            functools.partial(pack_upper_body, level=s, segs=segs, nsup=nsup),
            (1,),
            (meta, keep_rows),
            [(u_panels, pl.BlockSpec((1, nseg, rows, cols), lambda i, *_: (s, 0, 0, 0)))],
            [(shape((cols, (segs + last - s) * rows), BF16), None)],
        )[0]

    upper = upper_piece(last)
    ups = {last: chain_gather(upper, n_row)}
    (lower,) = call(
        functools.partial(pack_lower_body, blocks=blocks, halves=halves, blk=blk, nsup=nsup),
        (nsup,),
        (meta, keep_cols),
        [(after(l_t, upper), level_spec)],
        [(shape((nsup, rows, lw), BF16), pl.BlockSpec((1, rows, lw), lambda s, *_: (s, 0, 0)))],
    )
    low_last = lax.all_gather(lower[last:, :, :base_l], "col", axis=1, tiled=True)
    low_rest = lax.all_gather(lower[:last], "col", axis=1, tiled=True)
    region_t = after(region, upper).transpose(0, 2, 1, 3)
    out0 = jnp.pad(region_t, ((nsup, 0), (nsup, 0), (0, 0), (0, 0)))
    pair_spec = pl.BlockSpec((2, rows, base_l), lambda i, m: (0, i, 0))
    known = call(
        functools.partial(pack_region_body, blocks=blocks, halves=halves, blk=blk),
        (segs,),
        (meta,),
        [(region_t, pl.BlockSpec((1, aseg, rows, cols), lambda i, m: (m[0, i], 0, 0, 0)))],
        [(shape((2, base_k, base_l), BF16), pair_spec)],
    )
    known = known[0].reshape(2 * base_k, base_l)
    dims = (base_k, base_l, rows, cols)
    base_tiles, width_all = base_l // cols, rows * n_col
    lane = min(cols, 128)
    pieces = []
    xs, ys, ds, x_sups, sup_twos = {}, {}, {}, {}, {}
    gate = ups[last][1:]

    def level(s, out0, gate):
        steps = last - s
        nrow, ncol = base_k + steps * rows, base_l + steps * cols
        if s:
            ups[s - 1] = chain_gather(after(upper_piece(s - 1), gate), n_row)
        panel, entry = (low_last, 0) if s == last else (low_rest, s)
        cs, qs, dd = ([p[k] for p in pieces] for k in range(3))
        sup_list = [sup_twos[last - i] for i in range(1, steps)]

        def row_part(known, cs, qs, dd, sup_list):
            def tiles(k, depth, wide):
                return pl.BlockSpec((depth, cols), lambda t, h: (k, jnp.minimum(t, wide - 1)))

            inputs = [(known, tiles(k, base_k, base_tiles)) for k in range(2)]
            for i in range(steps):
                inputs += [(cs[i], None), (qs[i], tiles(0, 2 * rows, base_tiles + i)), (dd[i], None)]
            inputs += [(x, None) for x in sup_list]
            chunk = pl.BlockSpec((n_half, rows + CODES, cols), lambda t, h: (0, 0, t))
            keep = pl.BlockSpec((n_half, rows, cols), lambda t, h: (0, 0, t))
            return call(
                functools.partial(row_body, steps=steps, dims=dims, n_row=n_row, base_tiles=base_tiles),
                (base_tiles + steps,),
                (jnp.stack([row_at, bit]).astype(jnp.int32),),
                [(u, None) for u in ups[s]] + inputs,
                [
                    (shape((n_half, rows + CODES, ncol), jnp.int16), chunk),
                    (shape((n_half, rows, ncol), F32), keep),
                    (shape((width_all, nrow), BF16), None),
                ],
                [pltpu.VMEM((width_all, cols), F32)],
                limit=LARGE,
            )

        def col_part(js, coded):
            chunk = jnp.mod(row_at + jnp.array(js), n_row).astype(jnp.int32)
            outs = [
                (shape((len(js), base_k, cols), F32), pl.BlockSpec((1, base_k, cols), lambda i, c: (i, 0, 0)))
            ]
            outs += [(shape((base_k + CODES, cols), jnp.int16), None)] * coded
            return call(
                functools.partial(col_body, steps=steps, dims=dims, coded=coded),
                (len(js),),
                (chunk,),
                [(p, None) for p in [known] + cs]
                + [(panel, pl.BlockSpec((1, cols, ncol), lambda i, c: (entry, c[i], 0)))],
                outs,
                limit=LARGE,
            )

        def share_of(j):
            group, i = shares[j]
            return group, pl.BlockSpec((1, base_k, lane), lambda k, *_: (i, 0, k))

        def flow(j, arrived):
            return call(
                pass_body,
                (cols // lane,),
                (),
                [share_of(j), (arrived, pl.BlockSpec((base_k + CODES, lane), lambda k: (0, k)))],
                [
                    (
                        shape((base_k + CODES, cols), jnp.int16),
                        pl.BlockSpec((base_k + CODES, lane), lambda k: (0, k)),
                    )
                ],
            )[0]

        order = [n_row - 1, 1] + list(range(2, n_row - 1)) + [0]
        group, a, b = col_part(order, 2)
        x_sup = sup_two = None
        if steps:
            (share,) = call(
                functools.partial(side_body, steps=steps, dims=dims),
                (n_row,),
                (),
                [(x, None) for x in qs + after(dd, (a, b)) + sup_list]
                + [(panel, pl.BlockSpec((1, cols, ncol), lambda i: (entry, i, 0)))],
                [
                    (
                        shape((n_row, steps * rows + CODES, cols), jnp.int16),
                        pl.BlockSpec((1, steps * rows + CODES, cols), lambda i: (i, 0, 0)),
                    )
                ],
                limit=LARGE,
            )
            share = lax.all_to_all(share, "row", 0, 0)
            x_sup, sup_two = call(
                functools.partial(side_end_body, level=s, segs=segs, rows=rows),
                (1,),
                (keep_rows,),
                [(share, None)],
                [(shape((steps * rows, cols), F32), None), (shape((2 * steps * rows, cols), BF16), None)],
            )
            x_sups[s], sup_twos[s] = x_sup, sup_two
        shares = {j: (group, i) for i, j in enumerate(order)}
        for step in range(1, n_row):
            if step > 1:
                a = flow(n_row - step, flow_up)
                b = flow(step, flow_down)
            flow_up = lax.ppermute(a, "row", [(i, i + 1) for i in range(step)])
            flow_down = lax.ppermute(b, "row", [(i, i - 1) for i in range(n_row - step, n_row)])
            if step == 1:
                send, mine, up = row_part(after(known, (a, b)), cs, qs, dd, sup_list)
                got = lax.ppermute(send, "col", [(i, i ^ 1) for i in range(n_col)])
        chunk = pl.BlockSpec((1, rows + CODES, ncol), lambda i: (i, 0, 0))
        (half,) = call(
            join_body,
            (n_half,),
            (),
            [(mine, pl.BlockSpec((1, rows, ncol), lambda i: (i, 0, 0))), (got, chunk)],
            [(shape((n_half, rows + CODES, ncol), jnp.int16), chunk)],
        )
        groups = [[i for i in range(n_col) if i % 2 == b] for b in range(2)]
        swapped = lax.all_to_all(half, "col", 0, 0, axis_index_groups=groups)
        y, y_two = call(
            functools.partial(row_end_body, level=s, rows=rows, blk=blk),
            (1,),
            (keep_cols,),
            [(swapped, None)],
            [(shape((rows, ncol), F32), None), (shape((2 * rows, ncol), BF16), None)],
        )
        x_spec = pl.BlockSpec((base_k, lane), lambda k, *_: (0, k))
        coded_spec = pl.BlockSpec((base_k + CODES, lane), lambda k, *_: (0, k))
        x, x_two = call(
            functools.partial(col_end_body, level=s, rows=rows),
            (cols // lane,),
            (keep_rows,),
            [share_of(0), (after(flow_up, y), coded_spec), (flow_down, coded_spec)],
            [
                (shape((base_k, cols), F32), x_spec),
                (shape((2 * base_k, cols), BF16), pl.BlockSpec((2 * base_k, lane), lambda k, *_: (0, k))),
            ],
        )
        (share,) = call(
            functools.partial(diag_body, rows=rows),
            (1,),
            (),
            [(up, None), (x_two, None)] + ([(sup_two, None)] if steps else []),
            [(shape((n_col, rows + CODES, cols), jnp.int16), None)],
        )
        share = lax.all_to_all(share, "col", 0, 0)
        d, d_two = call(
            functools.partial(diag_end_body, rows=rows),
            (1,),
            (),
            [(diag_inv[s], None), (share, None)],
            [(shape((rows, cols), F32), None), (shape((2 * rows, cols), BF16), None)],
        )
        xs[s], ys[s], ds[s] = x, y, d
        pieces.append((x_two, y_two, d_two))
        return out0, x

    for s in reversed(range(nsup)):
        out0, gate = level(s, out0, gate)
    xs, ys, ds = ([v[s] for s in range(nsup)] for v in (xs, ys, ds))
    sups = [x_sups[s] for s in range(last)]
    anywhere = pl.BlockSpec(memory_space=pl.ANY)
    full = shape((nseg, nseg, rows, cols), F32)
    (out,) = call(
        functools.partial(put_cols_body, segs=segs, nsup=nsup, rows=rows),
        (aseg,),
        (meta,),
        [(v, None) for v in xs] + [(out0, anywhere)],
        [(full, pl.BlockSpec((1, nsup, rows, cols), lambda a, m: (nsup + a, 0, 0, 0)))],
        alias={1 + nsup: 0},
    )
    (out,) = call(
        functools.partial(
            put_rows_body, blocks=blocks, halves=halves, blk=blk, nsup=nsup, nseg=nseg, segs=segs, rows=rows
        ),
        (nsup,),
        (meta,),
        [(v, None) for v in ys + ds + sups] + [(out, anywhere)],
        [(full, pl.BlockSpec((1, nseg, rows, cols), lambda s, m: (s, 0, 0, 0)))],
        alias={3 * nsup: 0},
    )
    return out


def used_first(used):
    i = jnp.arange(used.shape[0], dtype=jnp.int32)
    before = jnp.sum(jnp.where(i[None, :] < i[:, None], used[None, :].astype(jnp.int32), 0), 1)
    place = jnp.where(used, before, jnp.sum(used.astype(jnp.int32)) + i - before)
    return jnp.sum(jnp.where(place[:, None] == i[None, :], i[:, None], 0), 0), place


def per_device(region, l_panels, u_panels, diag_inv, pattern, *, n_row, n_col, fractions):
    aseg, rows, _, cols = region.shape
    nsup, _ = u_panels.shape[:2]
    blk = min(BLK, cols)
    halves = cols // blk
    row_at, col_at = lax.axis_index("row"), lax.axis_index("col")
    cblk = col_at * rows // BLK
    rblk = row_at * cols // BLK
    used = jnp.max(pattern[:, nsup:], axis=0) > 0
    most_rows = jnp.max(jnp.sum(used, axis=0))
    per_row = used.reshape(aseg, n_row, -1)
    most_cols = jnp.max(jnp.sum(per_row, axis=(0, 2)))
    mine_r = pick(used, cblk, 1)
    mine_c = lax.dynamic_slice_in_dim(used, rblk, halves, 1).reshape(-1)
    seg_list, slot_of = used_first(mine_r)
    col_list, _ = used_first(mine_c)
    wide = aseg * halves
    fill = lambda v: jnp.pad(v, (0, wide - v.shape[0]))
    meta = jnp.stack([fill(seg_list), col_list // halves, col_list % halves, fill(slot_of)])
    l_t = l_panels.transpose(0, 2, 1, 3)
    caps = [(-(-aseg * a // 16), -(-wide * b // 16 // halves) * halves) for a, b in fractions]
    fits = [jnp.logical_and(most_rows <= a, most_cols <= b) for a, b in caps]
    choice = len(caps) - 1
    for i in reversed(range(len(caps) - 1)):
        choice = jnp.where(fits[i], i, choice)
    args = (region, l_t, u_panels, diag_inv, meta, pattern, cblk, rblk)
    makes = [
        functools.partial(branch, sizes=(n_row, n_col, halves, blk), segs=a, blocks=b)
        for a, b in caps
    ]
    out = lax.switch(choice, makes, *args) if len(makes) > 1 else makes[0](*args)
    return out.transpose(0, 2, 1, 3)


FRACTIONS = ((12, 12), (14, 12), (16, 16))


def solution(mesh):
    in_specs = (
        P(None, "col", None, "row"),
        P(None, "col", None, "row"),
        P(None, None, "col", "row"),
        P(None, "col", "row"),
        P(),
    )
    body = functools.partial(
        per_device, n_row=mesh.shape["row"], n_col=mesh.shape["col"], fractions=FRACTIONS
    )
    return jax.shard_map(
        body, mesh=mesh, in_specs=in_specs, out_specs=P(None, "col", None, "row"), check_vma=False
    )
```
